32 devices in a mesh: grp: 2 (over core), dp: 4 (over z), mp: 4 (over y, x).
Axes of the slice: x: 2, y: 2, z: 4, core: 2. Of those that a mesh axis runs over, the one named last changes fastest.
Arguments:
- hidden: bfloat16 [1024, 5120], P(('dp', 'mp')), may hold values from -6 to 6
- enc_weight: bfloat16 [5120, 8192], P(None, 'mp'), may hold values from -0.078125 to 0.078125
- enc_bias: bfloat16 [8192], P('mp'), may hold values from -5 to 5
- enc_frozen: bfloat16 [5120, 64], replicated, may hold values from -0.078125 to 0.078125
- enc_adapter: bfloat16 [64, 8192], P(None, 'mp'), may hold values from -0.75 to 0.75
- text_rows: bfloat16 [2560, 8192], P(('dp', 'mp')), may hold values from -6 to 6
- norm_gain: bfloat16 [8192], replicated, may hold values from 0.5 to 1.5
- value_weight: bfloat16 [8192, 1024], P(('dp', 'mp')), may hold values from -0.0625 to 0.0625
- value_bias: bfloat16 [1024], replicated, may hold values from -5 to 5
- llm_frozen: bfloat16 [8192, 64], P(('dp', 'mp')), may hold values from -0.0625 to 0.0625
- llm_adapter: bfloat16 [64, 1024], replicated, may hold values from -0.75 to 0.75
- targets: bfloat16 [2560, 1024], P(('dp', 'mp')), may hold values from -6 to 6
- dest_owner: int32 [1024, 1], replicated, may hold values from 0 to 15; in each aligned block of 256 rows (0 to 255, 256 to 511, ...) at most 32 rows name the same one
- seq_length: int32 [16], P(('dp', 'mp')), may hold values from 128 to 160
Outputs:
- grad_enc: float32 [64, 8192], P('grp', 'mp')
- grad_llm: float32 [64, 1024], P('grp')
The draws below stay inside these ranges and needn't reach their ends.
Inputs may be any that keep to these rules, and one draw needn't show every extreme that they name: `dest_owner`: within the tokens of one encoder block (aligned blocks of 256 rows) no LLM device is named more than 32 times, and some device is named exactly 32 times in some blocks.
All inputs are finite; a program needn't handle non-finite values.
Results may differ from the reference program's by a relative error of at most 0.003.
Values may be sent and summed in bfloat16 or wider, within the bound.
A program may use at most 128 MiB of HBM per device.

```python
import math
import jax
import jax.numpy as jnp
import numpy as np
from jax import lax

D = 8192
MH = 5120
KV = 1024
RANK = 64
ENC_DEV = 256
LLM_DEV = 160
OWNERS = 16
CAP = 32
IMG = 1024
N_DP = 4
N_MP = 4


def touch_ends(values, rng, low, top_value):
    shape = values.shape
    place = [jax.random.randint(jax.random.fold_in(rng, axis), (), 0, shape[axis]) for axis in range(len(shape))]
    values = values.at[tuple(place)].set(low)
    longest = shape.index(max(shape))
    place[longest] = (place[longest] + 1) % shape[longest]
    return values.at[tuple(place)].set(top_value)


def level_of(stream_key, dims, shards, low, top_value):
    def one(dim, parts):
        heights = jax.random.uniform(jax.random.fold_in(jax.random.fold_in(stream_key, 6), dim), (parts,), jnp.float32, low / len(shards), top_value / len(shards))
        return jnp.repeat(jnp.exp(heights), dims[dim] // parts).reshape((-1,) + (1,) * (len(dims) - dim - 1))

    factor_of = one(*shards[0])
    for cut in shards[1:]:
        factor_of = factor_of * one(*cut)
    return factor_of


def deal_out(key, own, number, rows, count, top, reach, slope):
    sequence = jax.random.permutation(key, count)
    heavy_load, common = shares(count, rows * top, reach, slope, True), shares(count, rows * top, reach, slope, False)
    places = jnp.arange(count)

    def named(sizes, offset_by):
        used = int((sizes > 0).sum())
        fixed = max(1, used // 4)
        moved = fixed + (places - fixed + offset_by * (used - fixed)) % max(1, count - fixed)
        return jnp.zeros((count,), jnp.int32).at[sequence[jnp.where(places < fixed, places, moved)]].set(jnp.asarray(sizes, jnp.int32))

    sizes = jnp.where(number % 4 == 0, named(heavy_load, number // 4), named(common, number - number // 4 - 1))
    mixed = jax.random.permutation(jax.random.fold_in(own, 3), count)
    donor, sink = mixed[0:count // 2 * 2:2], mixed[1:count // 2 * 2:2]
    room = jnp.minimum(sizes[donor] - 1, reach - sizes[sink]) // 2
    room = jnp.where((donor == sequence[0]) | (sink == sequence[0]) | (sizes[sink] == 0), 0, jnp.maximum(room, 0))
    moved = jax.random.randint(jax.random.fold_in(own, 4), (count // 2,), 0, 1 << 20) % (room + 1)
    sizes = sizes.at[donor].add(-moved).at[sink].add(moved)
    items = jnp.searchsorted(jnp.cumsum(sizes), jnp.arange(rows * top), side="right").astype(jnp.int32)
    listing = items.reshape(top, rows).T
    listing = listing[jax.random.permutation(jax.random.fold_in(own, 1), rows)]
    offset_by = jax.random.randint(jax.random.fold_in(own, 2), (rows, 1), 0, top)
    return jnp.take_along_axis(listing, (jnp.arange(top)[None, :] + offset_by) % top, axis=1)


def shares(number_of, total, most, slope, full):
    portions = [(1 << 20) // math.isqrt(grade ** slope) + 1 for grade in range(1, number_of + 1)]
    largest = most if full else min(most, max(-(-total // number_of), total * portions[0] // sum(portions)))
    least = 1 if total - largest >= number_of - 1 else 0
    given, surplus = [largest] + [least] * (number_of - 1), total - largest - least * (number_of - 1)
    while surplus > 0:
        candidates = [i for i in range(1, number_of) if given[i] < largest] or [i for i in range(1, number_of) if given[i] < most]
        pool, left = sum([portions[i] for i in candidates]), surplus
        for i in candidates:
            extra = min(most - given[i], max(1, left * portions[i] // pool), surplus)
            given[i] = given[i] + extra
            surplus = surplus - extra
    return np.array(given)


def noise(own_key, dims, scale, most, shards=(), kind=jnp.bfloat16):
    values = scale * jax.random.normal(own_key, dims, jnp.float32)
    if shards:
        values = values * level_of(own_key, dims, shards, -0.22, 0.18)
    return jnp.clip(values, -most, most).astype(kind)


def setup_inputs(seed: int = 0) -> dict:
    streams_of = jax.random.split(jax.random.key(seed), 15)
    hidden = noise(streams_of[0], (IMG, MH), 1.0, 6.0, ((0, 16),))
    enc_weight = noise(streams_of[1], (MH, D), MH ** -0.5, 0.078125, ((1, 4),))
    enc_bias = noise(streams_of[2], (D,), 1.0, 5.0, ((0, 4),))
    enc_frozen = noise(streams_of[3], (MH, RANK), MH ** -0.5, 0.078125)
    enc_adapter = noise(streams_of[4], (RANK, D), RANK ** -0.5, 0.75, ((1, 4),))
    text_rows = noise(streams_of[5], (OWNERS * LLM_DEV, D), 1.0, 6.0, ((0, 16),))
    norm_gain = jnp.clip(1.0 + 0.1 * jax.random.normal(streams_of[6], (D,), jnp.float32), 0.5, 1.5).astype(jnp.bfloat16)
    value_weight = noise(streams_of[7], (D, KV), D ** -0.5, 0.0625, ((0, 16),))
    value_bias = noise(streams_of[8], (KV,), 1.0, 5.0)
    llm_frozen = noise(streams_of[9], (D, RANK), D ** -0.5, 0.0625, ((0, 16),))
    llm_adapter = noise(streams_of[10], (RANK, KV), RANK ** -0.5, 0.75)
    targets = noise(streams_of[11], (OWNERS * LLM_DEV, KV), 1.0, 6.0, ((0, 16),))
    dest_owner_keys = jax.random.split(jax.random.fold_in(streams_of[12], 1), IMG // ENC_DEV)
    dest_owner_turns = jax.random.permutation(jax.random.fold_in(streams_of[12], 3), IMG // ENC_DEV)
    dest_owner = jax.vmap(lambda own, number: deal_out(jax.random.fold_in(streams_of[12], 2), own, number, ENC_DEV, OWNERS, 1, CAP, 2))(dest_owner_keys, dest_owner_turns).reshape((IMG, 1))
    seq_length = touch_ends(jax.random.randint(streams_of[13], (OWNERS,), N_DP * CAP, LLM_DEV + 1), jax.random.fold_in(streams_of[13], 1), N_DP * CAP, LLM_DEV).astype(jnp.int32)
    return dict(hidden=hidden, enc_weight=enc_weight, enc_bias=enc_bias, enc_frozen=enc_frozen, enc_adapter=enc_adapter, text_rows=text_rows, norm_gain=norm_gain, value_weight=value_weight, value_bias=value_bias, llm_frozen=llm_frozen, llm_adapter=llm_adapter, targets=targets, dest_owner=dest_owner, seq_length=seq_length)


epsilon = 1e-06

def reference(hidden, enc_weight, enc_bias, enc_frozen, enc_adapter, text_rows, norm_gain, value_weight, value_bias, llm_frozen, llm_adapter, targets, dest_owner, seq_length):
    owners = N_DP * N_MP
    enc_low = jnp.dot(hidden, enc_frozen, preferred_element_type=jnp.float32).astype(jnp.bfloat16)
    merged_rows = jnp.dot(hidden, enc_weight, preferred_element_type=jnp.float32) + enc_bias.astype(jnp.float32)
    merged_rows = (merged_rows + jnp.dot(enc_low, enc_adapter, preferred_element_type=jnp.float32)).astype(jnp.bfloat16)
    destiny = dest_owner[:, 0].reshape(N_DP, ENC_DEV)
    markers = (destiny[:, :, None] == jnp.arange(owners, dtype=jnp.int32)[None, None, :]).astype(jnp.int32)
    slot_rank = lax.optimization_barrier(jnp.sum((jnp.cumsum(markers, axis=1) - markers) * markers, axis=2))
    placing = destiny * LLM_DEV + slot_rank * N_DP + jnp.arange(N_DP, dtype=jnp.int32)[:, None]
    placing = placing.reshape(-1).astype(jnp.int32)
    all_rows = text_rows.at[placing].set(merged_rows)
    wide_rows = all_rows.astype(jnp.float32)
    inverse = lax.rsqrt(lax.optimization_barrier(jnp.mean(wide_rows * wide_rows, axis=1, keepdims=True)) + epsilon)
    gain_wide = norm_gain.astype(jnp.float32)
    normed = (wide_rows * inverse * gain_wide).astype(jnp.bfloat16)
    low_rank = jnp.dot(normed, llm_frozen, preferred_element_type=jnp.float32).astype(jnp.bfloat16)
    values_out = jnp.dot(normed, value_weight, preferred_element_type=jnp.float32) + value_bias.astype(jnp.float32)
    values_out = values_out + jnp.dot(low_rank, llm_adapter, preferred_element_type=jnp.float32)
    position = jnp.arange(owners * LLM_DEV, dtype=jnp.int32) % LLM_DEV
    length = jnp.repeat(seq_length, LLM_DEV)
    row_weight = jnp.where(position < length, 1.0 / length.astype(jnp.float32), 0.0).astype(jnp.float32)
    dvalues = ((values_out - targets.astype(jnp.float32)) * row_weight[:, None]).astype(jnp.bfloat16)
    grad_llm = jnp.dot(low_rank.T, dvalues, preferred_element_type=jnp.float32)
    low_grad = jnp.dot(dvalues, llm_adapter.T, preferred_element_type=jnp.float32).astype(jnp.bfloat16)
    picked_dv = dvalues[placing]
    picked_low = low_grad[placing]
    picked_rows = wide_rows[placing]
    picked_inverse = inverse[placing]
    dnormed = jnp.dot(picked_dv, value_weight.T, preferred_element_type=jnp.float32)
    dnormed = dnormed + jnp.dot(picked_low, llm_frozen.T, preferred_element_type=jnp.float32)
    scaled = gain_wide * dnormed
    cubed = picked_inverse * picked_inverse * picked_inverse
    image_grad = picked_inverse * scaled - picked_rows * cubed * lax.optimization_barrier(jnp.mean(scaled * picked_rows, axis=1, keepdims=True))
    image_grad = image_grad.astype(jnp.bfloat16)
    grad_enc = jnp.dot(enc_low.T, image_grad, preferred_element_type=jnp.float32)
    return (grad_enc, grad_llm)
```

```python
import jax
import jax.numpy as jnp
from jax import lax
from jax.sharding import PartitionSpec as P

epsilon = 1e-06
F32 = jnp.float32
BF16 = jnp.bfloat16


def swapped(array, axis, bit):
    return lax.ppermute(array, axis, [(i, i ^ 1 << bit) for i in range(lax.axis_size(axis))])


def summed(array, axis):
    for bit in range(lax.axis_size(axis).bit_length() - 1):
        array = array + swapped(array, axis, bit)
    return array


def slot_ranks(destiny, owners):
    markers = (destiny[:, None] == jnp.arange(owners, dtype=jnp.int32)[None, :]).astype(jnp.int32)
    return jnp.sum((jnp.cumsum(markers, axis=0) - markers) * markers, axis=1)


def body(
    hidden,
    enc_weight,
    enc_bias,
    enc_frozen,
    enc_adapter,
    text_rows,
    norm_gain,
    value_weight,
    value_bias,
    llm_frozen,
    llm_adapter,
    targets,
    dest_owner,
    seq_length,
):
    data_ways = lax.axis_size("dp")
    model_ways = lax.axis_size("mp")
    owners = data_ways * model_ways
    core = lax.axis_index("grp")
    lead = core == 0
    block = lax.axis_index("dp")
    member = lax.axis_index("mp")
    owner_index = block * model_ways + member
    own_tokens = hidden.shape[0]
    block_tokens = own_tokens * model_ways
    capacity = 2 * block_tokens // owners
    area = capacity * data_ways
    llm_rows, model_width = text_rows.shape
    rank = enc_frozen.shape[1]
    kv_half = llm_adapter.shape[1] // 2
    col_half = enc_weight.shape[1] // 2

    def half_of(array, axis):
        size = array.shape[axis] // 2
        return lax.dynamic_slice_in_dim(array, core * size, size, axis)

    def in_order(mine, other):
        return jnp.where(lead, mine, other), jnp.where(lead, other, mine)

    part = lax.all_gather(half_of(hidden, 0), "mp", axis=0, tiled=False)
    padding = -(kv_half + rank) % 128
    packed = jnp.concatenate(
        [half_of(value_weight, 1), llm_frozen, jnp.zeros((llm_frozen.shape[0], padding), BF16)],
        axis=1,
    )
    packed, part = lax.optimization_barrier((packed, part))
    weights = lax.all_gather(packed, ("dp", "mp"), axis=0, tiled=True)

    group_rows = jnp.stack(in_order(part, swapped(part, "grp", 0)), axis=1)
    group_rows = group_rows.reshape(block_tokens, hidden.shape[1])
    enc_low = jnp.dot(group_rows, enc_frozen, preferred_element_type=F32).astype(BF16)
    merged = jnp.dot(group_rows, half_of(enc_weight, 1), preferred_element_type=F32)
    merged = merged + half_of(enc_bias, 0).astype(F32)
    merged = merged + jnp.dot(enc_low, half_of(enc_adapter, 1), preferred_element_type=F32)
    merged = merged.astype(BF16).reshape(model_ways, own_tokens, col_half)
    own_cols = lax.all_to_all(merged, "mp", split_axis=0, concat_axis=0, tiled=True)
    first, second = in_order(own_cols, swapped(own_cols, "grp", 0))
    image = jnp.concatenate(
        [piece[k] for k in range(model_ways) for piece in (first, second)], axis=1
    )

    own_targets = half_of(targets, 1)
    head = own_targets[:area].reshape(capacity, data_ways, kv_half)
    head = lax.all_to_all(head, "dp", split_axis=1, concat_axis=1, tiled=True)
    table = lax.all_gather(head, "mp", axis=0, tiled=False)
    table = table.reshape(model_ways * area, kv_half)
    lengths = lax.all_gather(seq_length.astype(F32), ("dp", "mp"), axis=0, tiled=True)
    destiny = dest_owner[:, 0]
    block_dest = lax.dynamic_slice_in_dim(destiny, block * block_tokens, block_tokens)
    block_slot = slot_ranks(block_dest, owners)
    dest = lax.dynamic_slice_in_dim(block_dest, member * own_tokens, own_tokens)
    slot = lax.dynamic_slice_in_dim(block_slot, member * own_tokens, own_tokens)
    index = (dest % model_ways * capacity + slot) * data_ways + dest // model_ways
    picker = (index[:, None] == jnp.arange(model_ways * area, dtype=jnp.int32)[None, :]).astype(BF16)
    image_targets = jnp.dot(picker, table, preferred_element_type=F32)
    owner_marks = dest[:, None] == jnp.arange(owners, dtype=jnp.int32)[None, :]
    image_length = jnp.sum(jnp.where(owner_marks, lengths[None, :], 0.0), axis=1)
    image_place = (slot * data_ways + block).astype(F32)
    image_weight = jnp.where(image_place < image_length, 1.0 / image_length, 0.0)

    counts = jnp.sum(
        (destiny.reshape(data_ways, block_tokens) == owner_index).astype(jnp.int32), axis=1
    )
    position = jnp.arange(llm_rows, dtype=jnp.int32)
    marks = position[:, None] % data_ways == jnp.arange(data_ways, dtype=jnp.int32)[None, :]
    row_count = jnp.sum(jnp.where(marks, counts[None, :], 0), axis=1)
    replaced = (position < area) & (position // data_ways < row_count)
    length = seq_length[0]
    text_weight = jnp.where(
        (position < length) & ~replaced, 1.0 / length.astype(F32), 0.0
    )
    row_weight = jnp.concatenate([image_weight, text_weight])

    gain = norm_gain.astype(F32)

    def norm(rows):
        wide = rows.astype(F32)
        inverse = lax.rsqrt(jnp.mean(wide * wide, axis=1, keepdims=True) + epsilon)
        return (wide * inverse * gain).astype(BF16), inverse

    image_normed, inverse = norm(image)
    text_normed, _ = norm(text_rows)
    normed = jnp.concatenate([image_normed, text_normed], axis=0)
    product = jnp.dot(normed, weights, preferred_element_type=F32)
    low = product[:, kv_half : kv_half + rank].astype(BF16)
    adapter = half_of(llm_adapter, 1)
    values = product[:, :kv_half] + half_of(value_bias, 0).astype(F32)
    values = values + jnp.dot(low, adapter, preferred_element_type=F32)
    all_targets = jnp.concatenate([image_targets, own_targets.astype(F32)], axis=0)
    dvalues = ((values - all_targets) * row_weight[:, None]).astype(BF16)
    grad_llm = jnp.dot(low.T, dvalues, preferred_element_type=F32)

    image_dv = dvalues[:own_tokens]
    dlow = jnp.dot(image_dv, adapter.T, preferred_element_type=F32)
    dlow = (dlow + swapped(dlow, "grp", 0)).astype(BF16)
    dlow = jnp.where(lead, dlow, jnp.zeros_like(dlow))
    sides = jnp.concatenate([image_dv, dlow, jnp.zeros((own_tokens, padding), BF16)], axis=1)
    dnormed = lax.dot_general(
        sides, weights, (((1,), (1,)), ((), ())), preferred_element_type=F32
    )
    pieces = [dnormed[:, k * col_half : (k + 1) * col_half] for k in range(2 * model_ways)]
    even, odd = jnp.stack(pieces[0::2]), jnp.stack(pieces[1::2])
    kept, given = in_order(even, odd)
    dnormed = kept + swapped(given, "grp", 0)
    halves = gain.reshape(model_ways, 2, col_half)
    own_gain = jnp.where(lead, halves[:, 0], halves[:, 1])
    scaled = own_gain[:, None, :] * dnormed
    own_wide = own_cols.astype(F32)
    total = jnp.sum(scaled * own_wide, axis=(0, 2))
    average = ((total + swapped(total, "grp", 0)) / model_width)[None, :, None]
    inv = inverse[None]
    dimage = (inv * scaled - own_wide * (inv * inv * inv) * average).astype(BF16)
    back = lax.all_to_all(dimage, "mp", split_axis=0, concat_axis=0, tiled=True)
    grad_enc = jnp.dot(
        enc_low.T, back.reshape(block_tokens, col_half), preferred_element_type=F32
    )

    grad_llm = summed(grad_llm, "mp")
    grads = summed(jnp.concatenate([grad_enc, grad_llm], axis=1), "dp")
    upper, lower = grads[: rank // 2], grads[rank // 2 :]
    kept, given = in_order(upper, lower)
    first, second = in_order(kept, swapped(given, "grp", 0))
    return (
        jnp.concatenate([first[:, :col_half], second[:, :col_half]], axis=1),
        jnp.concatenate([first[:, col_half:], second[:, col_half:]], axis=1),
    )


def solution(mesh):
    return jax.shard_map(
        body,
        mesh=mesh,
        in_specs=(
            P(("dp", "mp"), None),
            P(None, "mp"),
            P("mp"),
            P(),
            P(None, "mp"),
            P(("dp", "mp"), None),
            P(),
            P(("dp", "mp"), None),
            P(),
            P(("dp", "mp"), None),
            P(),
            P(("dp", "mp"), None),
            P(),
            P(("dp", "mp")),
        ),
        out_specs=(P("grp", "mp"), P("grp", None)),
        check_vma=False,
    )
```
